256 devices in a mesh: gz: 64 (over z, y, core), xy: 4 (over x).
Axes of the slice: x: 4, y: 4, z: 8, core: 2. Of those that a mesh axis runs over, the one named last changes fastest.
Arguments:
- image: float32 [512, 512, 512], P('gz', 'xy'), may hold values from -6 to 6
- offsets: int32 [4, 512, 4, 4], P(None, 'gz', 'xy'), may hold values from -6 to 6
- frac_index: int32 [4, 512, 4, 4], P(None, 'gz', 'xy'), may hold values from 0 to 15
- fractions: float32 [16, 3], replicated, may hold values from 0 to 1
Outputs:
- transported: float32 [512, 512, 512], P('gz', 'xy')
The draws below stay inside these ranges and needn't reach their ends.
All inputs are finite; a program needn't handle non-finite values.
Results may differ from the reference program's by a relative error of at most 0.0003.
Values sent between devices are 32-bit elements; how exact they have to be, the bound alone decides.
No kernel may reach another device: no remote copies, remote signals or barrier semaphores. Data moves between devices by JAX's collectives and lax.ppermute only.
A program may use at most 128 MiB of HBM per device.

```python
import jax
import jax.numpy as jnp
from jax import lax

BLOCK = 128
NBY = 4
STEPS = 4
FRACS = 16
NX = 512
NY = 512
NZ = 512


def place_ends(values, rng, least, top_value):
    spot = [jax.random.randint(jax.random.fold_in(rng, axis), (), 0, length) for axis, length in enumerate(values.shape)]
    widest = values.shape.index(max(values.shape))
    neighbour = spot[:widest] + [(spot[widest] + 1) % values.shape[widest]] + spot[widest + 1:]
    return values.at[tuple(spot)].set(least).at[tuple(neighbour)].set(top_value)


def block_levels(own_key, shape, cuts, low, largest):
    def one(axis_at, blocks):
        draws = jax.random.uniform(jax.random.fold_in(jax.random.fold_in(own_key, 6), axis_at), (blocks,), jnp.float32, low / len(cuts), largest / len(cuts))
        return jnp.repeat(jnp.exp(draws), shape[axis_at] // blocks).reshape((-1,) + (1,) * (len(shape) - axis_at - 1))

    loudness = one(*cuts[0])
    for cut in cuts[1:]:
        loudness = loudness * one(*cut)
    return loudness


def gaussian(stream_key, shape, width, limit, pieces=(), kind=jnp.bfloat16):
    values = jax.random.normal(stream_key, shape, jnp.float32) * width
    if len(pieces) > 0:
        values = block_levels(stream_key, shape, pieces, -0.22, 0.18) * values
    return jnp.clip(values, min=-limit, max=limit).astype(kind)


def setup_inputs(seed: int = 0) -> dict:
    key_list = jax.random.split(jax.random.key(seed), 5)
    return {
        "image": gaussian(key_list[0], (NZ, NX, NY), 1.0, 6.0, ((0, 64), (1, 4)), jnp.float32),
        "offsets": place_ends(jax.random.randint(key_list[1], (STEPS, NZ, NX // BLOCK, NBY), -6, 7), jax.random.fold_in(key_list[1], 1), -6, 6).astype(jnp.int32),
        "frac_index": place_ends(jax.random.randint(key_list[2], (STEPS, NZ, NX // BLOCK, NBY), 0, FRACS), jax.random.fold_in(key_list[2], 1), 0, FRACS - 1).astype(jnp.int32),
        "fractions": jnp.clip(jax.random.uniform(key_list[3], (FRACS, 3), jnp.float32, 0.0, 1.0), 0.0, 1.0),
    }


def cubic_weights(shares):
    return (-shares * (shares - 1.0) * (shares - 2.0) / 6.0,
            (shares + 1.0) * (shares - 1.0) * (shares - 2.0) / 2.0,
            -(shares + 1.0) * shares * (shares - 2.0) / 2.0,
            (shares + 1.0) * shares * (shares - 1.0) / 6.0)


def reference(image, offsets, frac_index, fractions):
    current = image
    block_rows = NX // BLOCK
    levels = jnp.arange(NZ, dtype=jnp.int32)
    for step_index in range(STEPS):
        padded = jnp.pad(current, ((0, 0), (2, 2), (2, 2)), mode="wrap")
        shifts_all = offsets[step_index]
        index_all = frac_index[step_index]

        def one_block(block_id):
            row_index = block_id // NBY
            col_index = block_id % NBY
            sub_volume = lax.dynamic_slice(padded, (jnp.int32(0), row_index * BLOCK, col_index * BLOCK), (NZ, BLOCK + 4, BLOCK + 4))
            shifts_now = shifts_all[:, row_index, col_index]
            picked = fractions[index_all[:, row_index, col_index]]
            zweights = cubic_weights(1.0 - picked[:, 0])
            xweights = cubic_weights(1.0 - picked[:, 1])
            yweights = cubic_weights(1.0 - picked[:, 2])
            merged = jnp.zeros((NZ, BLOCK + 4, BLOCK + 4), jnp.float32)
            for node in range(4):
                source = jnp.mod(levels - shifts_now - 2 + node, NZ).astype(jnp.int32)
                merged = merged + zweights[node][:, None, None] * sub_volume[source]
            along_y = jnp.zeros((NZ, BLOCK + 4, BLOCK), jnp.float32)
            for node in range(4):
                along_y = along_y + yweights[node][:, None, None] * merged[:, :, node:node + BLOCK]
            along_x = jnp.zeros((NZ, BLOCK, BLOCK), jnp.float32)
            for node in range(4):
                along_x = along_x + xweights[node][:, None, None] * along_y[:, node:node + BLOCK, :]
            return along_x

        blocks = lax.map(one_block, jnp.arange(block_rows * NBY, dtype=jnp.int32))
        current = blocks.reshape(block_rows, NBY, NZ, BLOCK, BLOCK).transpose(2, 0, 3, 1, 4).reshape(NZ, NX, NY)
    return current
```

```python
import jax
import jax.numpy as jnp
from jax import lax
from jax.experimental import pallas as pl
from jax.experimental.pallas import tpu as pltpu
from jax.sharding import PartitionSpec as P

REACH = 8
LANES = 128


def cubic_weights(shares):
    return (
        -shares * (shares - 1.0) * (shares - 2.0) / 6.0,
        (shares + 1.0) * (shares - 1.0) * (shares - 2.0) / 2.0,
        -(shares + 1.0) * shares * (shares - 2.0) / 2.0,
        (shares + 1.0) * shares * (shares - 1.0) / 6.0,
    )


def weight_table(fractions):
    parts = [jnp.stack(cubic_weights(1.0 - fractions[:, axis]), axis=1) for axis in range(3)]
    return jnp.concatenate(parts, axis=1).reshape(-1)


def advect_body(planes, rows, per_step, off_ref, idx_ref, tab_ref, up, own, down, rim_up, rim_own, rim_down, out_ref, win, line, sems):
    blocks = win.shape[2] // LANES

    @pl.when(pl.program_id(0) == 0)
    def _():
        pieces = [
            (up, 0, REACH, 8, rows),
            (own, REACH, planes, 8, rows),
            (down, REACH + planes, REACH, 8, rows),
            (rim_up, 0, REACH, 0, 8),
            (rim_own, REACH, planes, 0, 8),
            (rim_down, REACH + planes, REACH, 0, 8),
        ]
        copies = [
            pltpu.make_async_copy(src, win.at[pl.ds(first, count), pl.ds(row, height), :], sems.at[i])
            for i, (src, first, count, row, height) in enumerate(pieces)
        ]
        for copy in copies:
            copy.start()
        for copy in copies:
            copy.wait()

    lane = lax.broadcasted_iota(jnp.int32, (8, LANES), 1)
    from_right = lane < 64
    last_two = lane >= LANES - 2
    last_one = lane >= LANES - 1
    first_one = lane == 0
    tiles = rows // 8 + 1

    def plane(local, carry):
        k = pl.program_id(0) * per_step + local
        for b in range(blocks):
            left = ((b - 1) % blocks) * LANES
            right = ((b + 1) % blocks) * LANES
            base = k - off_ref[k * blocks + b] + (REACH - 2)
            entry = idx_ref[k * blocks + b] * 12
            cz = [tab_ref[entry + n] for n in range(4)]
            cx = [tab_ref[entry + 4 + n] for n in range(4)]
            cy = [tab_ref[entry + 8 + n] for n in range(4)]
            for t in range(tiles):
                here = pl.ds(t * 8, 8)
                mid = None
                edge = None
                for n in range(4):
                    m = cz[n] * win[base + n, here, pl.ds(b * LANES, LANES)]
                    e = cz[n] * jnp.where(
                        from_right,
                        win[base + n, here, pl.ds(right, LANES)],
                        win[base + n, here, pl.ds(left, LANES)],
                    )
                    mid = m if mid is None else mid + m
                    edge = e if edge is None else edge + e
                y = cy[2] * mid
                y = y + cy[0] * pltpu.roll(jnp.where(last_two, edge, mid), 2, 1)
                y = y + cy[1] * pltpu.roll(jnp.where(last_one, edge, mid), 1, 1)
                y = y + cy[3] * pltpu.roll(jnp.where(first_one, edge, mid), LANES - 1, 1)
                line[b, here, :] = y
                if t == 0:
                    line[b, pl.ds(tiles * 8, 8), :] = y
            for t in range(1, tiles):
                acc = cx[0] * line[b, pl.ds(t * 8 - 2, 8), :]
                for n in range(1, 4):
                    acc = acc + cx[n] * line[b, pl.ds(t * 8 - 2 + n, 8), :]
                out_ref[local, pl.ds((t - 1) * 8, 8), pl.ds(b * LANES, LANES)] = acc
        return carry

    lax.fori_loop(0, per_step, plane, 0)


def advect(up, own, down, rim_up, rim_own, rim_down, offsets, index, table, per_step):
    planes, rows, width = own.shape
    blocks = width // LANES

    def body(*refs):
        advect_body(planes, rows, per_step, *refs)

    anywhere = pl.BlockSpec(memory_space=pl.ANY)
    return pl.pallas_call(
        body,
        out_shape=jax.ShapeDtypeStruct(own.shape, jnp.float32),
        grid_spec=pltpu.PrefetchScalarGridSpec(
            num_scalar_prefetch=3,
            grid=(planes // per_step,),
            in_specs=[anywhere] * 6,
            out_specs=pl.BlockSpec((per_step, rows, width), lambda i, *_: (i, 0, 0)),
            scratch_shapes=[
                pltpu.VMEM((planes + 2 * REACH, rows + 8, width), jnp.float32),
                pltpu.VMEM((blocks, rows + 16, LANES), jnp.float32),
                pltpu.SemaphoreType.DMA((6,)),
            ],
        ),
        name="advect",
    )(offsets, index, table, up, own, down, rim_up, rim_own, rim_down)


def shifted(x, axis, by):
    devices = lax.axis_size(axis)
    return lax.ppermute(x, axis, [(i, (i + by) % devices) for i in range(devices)])


def local(image, offsets, frac_index, fractions):
    planes, rows, width = image.shape
    table = weight_table(fractions)
    current = image
    for step in range(offsets.shape[0]):
        up = shifted(current, "gz", 1)
        down = shifted(current, "gz", -1)
        above = shifted(current[:, rows - 2 :], "xy", 1)
        below = shifted(current[:, :2], "xy", -1)
        rim = jnp.concatenate([below, jnp.zeros((planes, 4, width), jnp.float32), above], axis=1)
        rim_up = shifted(rim, "gz", 1)
        rim_down = shifted(rim, "gz", -1)
        current = advect(
            up, current, down, rim_up, rim, rim_down,
            offsets[step].reshape(-1), frac_index[step].reshape(-1), table, 1,
        )
    return current


def solution(mesh):
    in_specs = (P("gz", "xy", None), P(None, "gz", "xy", None), P(None, "gz", "xy", None), P())
    out_specs = P("gz", "xy", None)
    return jax.shard_map(local, mesh=mesh, in_specs=in_specs, out_specs=out_specs, check_vma=False)
```

```python
import jax
import jax.numpy as jnp
from jax import lax
from jax.experimental import pallas as pl
from jax.experimental.pallas import tpu as pltpu
from jax.sharding import PartitionSpec as P


REACH = 8
LANES = 128
TILE = 8
MARGIN = 8


def cubic_weights(shares):
    return (
        -shares * (shares - 1.0) * (shares - 2.0) / 6.0,
        (shares + 1.0) * (shares - 1.0) * (shares - 2.0) / 2.0,
        -(shares + 1.0) * shares * (shares - 2.0) / 2.0,
        (shares + 1.0) * shares * (shares - 1.0) / 6.0,
    )


def weight_table(fractions):
    parts = [jnp.stack(cubic_weights(1.0 - fractions[:, axis]), axis=1) for axis in range(3)]
    return jnp.concatenate(parts, axis=1).reshape(-1)


def sweep(step, pieces, moves, tiles, targets, tags, table, ends=(), finish=None):
    planes, _, width = pieces[0][1].shape
    blocks = width // LANES
    inputs = [part for piece in pieces for part in piece]
    if finish:
        whole, first, middle = finish
        inputs.append(middle)
        after = first + middle.shape[1]

    def body(tag_ref, tab_ref, *refs):
        sources = refs[: len(inputs)]
        outputs = refs[len(inputs) : len(inputs) + 1 + len(ends)]
        win, line, *more = refs[len(inputs) + 1 + len(ends) :]
        out_ref = outputs[0]
        if finish:
            out_ref, sems = more
            last = pltpu.make_async_copy(sources[-1], outputs[0].at[:, pl.ds(first, after - first), :], sems.at[0])
            last.start()

        def drains(k):
            return [
                pltpu.make_async_copy(
                    out_ref.at[k, pl.ds(row, height), :], outputs[0].at[k, pl.ds(row, height), :], sems.at[1 + 2 * k + i]
                )
                for i, (row, height) in enumerate([(0, first), (after, whole - after)])
            ]

        def fill(p, carry):
            for piece, row, at, height in moves:
                for part in range(3):
                    win[part * planes + p, pl.ds(at, height), :] = sources[3 * piece + part][p, pl.ds(row, height), :]
            return carry

        lax.fori_loop(0, planes, fill, 0)
        lane = lax.broadcasted_iota(jnp.int32, (TILE, LANES), 1)
        from_right = lane < LANES // 2
        last_two = lane >= LANES - 2
        last_one = lane >= LANES - 1
        first_one = lane == 0

        def plane(k, carry):
            for b in range(blocks):
                here = pl.ds(b * LANES, LANES)
                left = pl.ds(((b - 1) % blocks) * LANES, LANES)
                right = pl.ds(((b + 1) % blocks) * LANES, LANES)
                tag = (step * planes + k) * blocks + b
                base = k - tag_ref[0, tag] + (REACH - 2)
                entry = tag_ref[1, tag] * 12
                cz = [tab_ref[entry + n] for n in range(4)]
                cx = [tab_ref[entry + 4 + n] for n in range(4)]
                cy = [tab_ref[entry + 8 + n] for n in range(4)]
                for t in range(tiles):
                    rows = pl.ds(t * TILE, TILE)
                    mid = None
                    edge = None
                    for n in range(4):
                        m = cz[n] * win[base + n, rows, here]
                        e = cz[n] * jnp.where(from_right, win[base + n, rows, right], win[base + n, rows, left])
                        mid = m if mid is None else mid + m
                        edge = e if edge is None else edge + e
                    y = cy[2] * mid
                    y = y + cy[0] * pltpu.roll(jnp.where(last_two, edge, mid), 2, 1)
                    y = y + cy[1] * pltpu.roll(jnp.where(last_one, edge, mid), 1, 1)
                    y = y + cy[3] * pltpu.roll(jnp.where(first_one, edge, mid), LANES - 1, 1)
                    line[b, rows, :] = y
                for t, row in targets:
                    acc = cx[0] * line[b, pl.ds(t * TILE - 2, TILE), :]
                    for n in range(1, 4):
                        acc = acc + cx[n] * line[b, pl.ds(t * TILE - 2 + n, TILE), :]
                    out_ref[k, pl.ds(row, TILE), here] = acc
                    for end, end_ref in zip(ends, outputs[1:]):
                        if t == end:
                            end_ref[k, :, here] = acc
            if finish:
                for copy in drains(k):
                    copy.start()
            return carry

        lax.fori_loop(0, planes, plane, 0)
        if finish:
            last.wait()
            for k in range(planes):
                for copy in drains(k):
                    copy.wait()

    inside = pl.BlockSpec(memory_space=pltpu.VMEM)
    scalars = pl.BlockSpec(memory_space=pltpu.SMEM)
    scratch = [
        pltpu.VMEM((3 * planes, tiles * TILE, width), jnp.float32),
        pltpu.VMEM((blocks, tiles * TILE, LANES), jnp.float32),
    ]
    if finish:
        out_shape = jax.ShapeDtypeStruct((planes, whole, width), jnp.float32)
        out_specs = pl.BlockSpec(memory_space=pl.ANY)
        scratch += [
            pltpu.VMEM((planes, whole, width), jnp.float32),
            pltpu.SemaphoreType.DMA((1 + 2 * planes,)),
        ]
    else:
        height = max(row for _, row in targets) + TILE
        out_shape = [jax.ShapeDtypeStruct((planes, height, width), jnp.float32)]
        out_shape += [jax.ShapeDtypeStruct((planes, TILE, width), jnp.float32)] * len(ends)
        out_specs = [inside] * len(out_shape)
    return pl.pallas_call(
        body,
        out_shape=out_shape,
        in_specs=[scalars] * 2 + [inside] * len(inputs),
        out_specs=out_specs,
        scratch_shapes=scratch,
        compiler_params=pltpu.CompilerParams(vmem_limit_bytes=14 << 20),
        name="sweep",
    )(tags, table, *inputs)


def shifted(x, axis, by):
    devices = lax.axis_size(axis)
    return lax.ppermute(x, axis, [(i, (i + by) % devices) for i in range(devices)])


def stacked(x):
    up = shifted(x, "gz", 1)
    down = shifted(x, "gz", -1)
    return up, x, down


def rim_of(first, last):
    above = shifted(last, "xy", 1)
    below = shifted(first, "xy", -1)
    row = lax.broadcasted_iota(jnp.int32, above.shape, 1)
    return jnp.where(row < TILE // 2, below, above)


def advance(image, offsets, frac_index, fractions):
    rows = image.shape[1]
    steps = offsets.shape[0]
    table = weight_table(fractions)
    tags = jnp.stack([offsets.reshape(-1), frac_index.reshape(-1)])
    margin = MARGIN
    centre = image[:, margin : rows - margin]
    first, last = image[:, :TILE], image[:, rows - TILE :]
    outer = None
    for step in range(steps):
        rim = rim_of(first, last)
        if outer is None:
            outer = jnp.concatenate([image[:, rows - margin :], rim, image[:, :margin]], axis=1)
        else:
            outer = lax.dynamic_update_slice(outer, rim, (0, margin, 0))
        inner = stacked(centre)
        outside = stacked(outer)
        tall = rows - 2 * margin
        many = margin // TILE
        margin += TILE
        (centre,) = sweep(
            step, [inner], [(0, 0, 0, tall)], tall // TILE,
            [(t, (t - 1) * TILE) for t in range(1, tall // TILE - 1)], tags, table,
        )
        moves = [(0, tall - 16, 0, 16), (1, 0, 16, 2 * margin - TILE), (0, 0, 8 + 2 * margin, 16)]
        upper, lower = range(1, many + 2), range(many + 3, 2 * many + 4)
        if step < steps - 1:
            outer, last, first = sweep(
                step, [inner, outside], moves, 2 * many + 5,
                [(t, (t - 1) * TILE) for t in (*upper, *lower)], tags, table,
                ends=(many + 1, many + 3),
            )
        else:
            targets = [(t, rows - margin + (t - 1) * TILE) for t in upper]
            targets += [(t, (t - many - 3) * TILE) for t in lower]
            image = sweep(
                step, [inner, outside], moves, 2 * many + 5, targets, tags, table,
                finish=(rows, margin, centre),
            )
    return image


def solution(mesh):
    in_specs = (P("gz", "xy", None), P(None, "gz", "xy", None), P(None, "gz", "xy", None), P())
    out_specs = P("gz", "xy", None)
    return jax.shard_map(advance, mesh=mesh, in_specs=in_specs, out_specs=out_specs, check_vma=False)
```

```python
import jax
import jax.numpy as jnp
from jax import lax
from jax.experimental import pallas as pl
from jax.experimental.pallas import tpu as pltpu
from jax.sharding import PartitionSpec as P


REACH = 8
LANES = 128
TILE = 8
MARGIN = 16


def cubic_weights(shares):
    return (
        -shares * (shares - 1.0) * (shares - 2.0) / 6.0,
        (shares + 1.0) * (shares - 1.0) * (shares - 2.0) / 2.0,
        -(shares + 1.0) * shares * (shares - 2.0) / 2.0,
        (shares + 1.0) * shares * (shares - 1.0) / 6.0,
    )


def weight_table(fractions):
    parts = [jnp.stack(cubic_weights(1.0 - fractions[:, axis]), axis=1) for axis in range(3)]
    return jnp.concatenate(parts, axis=1).reshape(-1)


def sweep(step, pieces, moves, tiles, targets, tags, table, ends=(), rim=None, finish=None):
    planes, _, width = pieces[0][1].shape
    blocks = width // LANES
    inputs = [part for piece in pieces for part in piece]
    if finish:
        whole, first, middle = finish
        inputs.append(middle)
        after = first + middle.shape[1]

    def body(tag_ref, tab_ref, *refs):
        sources = refs[: len(inputs)]
        outputs = refs[len(inputs) : len(inputs) + 1 + len(ends)]
        win, line, brim, *more = refs[len(inputs) + 1 + len(ends) :]
        out_ref = outputs[0]
        if finish:
            out_ref, sems = more
            last = pltpu.make_async_copy(sources[-1], outputs[0].at[:, pl.ds(first, after - first), :], sems.at[0])
            last.start()

        def drains(k):
            return [
                pltpu.make_async_copy(
                    out_ref.at[k, pl.ds(row, height), :], outputs[0].at[k, pl.ds(row, height), :], sems.at[1 + 2 * k + i]
                )
                for i, (row, height) in enumerate([(0, first), (after, whole - after)])
            ]

        odd = tag_ref[6, 0]
        starts = [planes, 2 * planes * (1 - odd), 2 * planes * odd]

        def fill(p, carry):
            for piece, row, at, height in moves:
                for part in range(3):
                    win[starts[part] + p, pl.ds(at, height), :] = sources[3 * piece + part][p, pl.ds(row, height), :]
            return carry

        lax.fori_loop(0, planes, fill, 0)
        lane = lax.broadcasted_iota(jnp.int32, (TILE, LANES), 1)
        from_right = lane < LANES // 2
        last_two = lane >= LANES - 2
        last_one = lane >= LANES - 1
        first_one = lane == 0

        from_below = lax.broadcasted_iota(jnp.int32, (TILE, LANES), 0) < TILE // 2

        def chosen(k, b, kind):
            tag = (step * planes + k) * blocks + b
            entry = tag_ref[2 * kind + 1, tag] * 12
            weights = [[tab_ref[entry + 4 * axis + n] for n in range(4)] for axis in range(3)]
            return k - tag_ref[2 * kind, tag] + (REACH - 2), weights

        def along_y(base, cz, cy, b, t):
            rows = pl.ds(t * TILE, TILE)
            here = pl.ds(b * LANES, LANES)
            left = pl.ds(((b - 1) % blocks) * LANES, LANES)
            right = pl.ds(((b + 1) % blocks) * LANES, LANES)
            mid = None
            edge = None
            for n in range(4):
                m = cz[n] * win[base + n, rows, here]
                e = cz[n] * jnp.where(from_right, win[base + n, rows, right], win[base + n, rows, left])
                mid = m if mid is None else mid + m
                edge = e if edge is None else edge + e
            y = cy[2] * mid
            y = y + cy[0] * pltpu.roll(jnp.where(last_two, edge, mid), 2, 1)
            y = y + cy[1] * pltpu.roll(jnp.where(last_one, edge, mid), 1, 1)
            return y + cy[3] * pltpu.roll(jnp.where(first_one, edge, mid), LANES - 1, 1)

        def along_x(lines, cx, b, row):
            acc = cx[0] * lines[b, pl.ds(row - 2, TILE), :]
            for n in range(1, 4):
                acc = acc + cx[n] * lines[b, pl.ds(row - 2 + n, TILE), :]
            return acc

        def plane(k, carry):
            for b in range(blocks):
                here = pl.ds(b * LANES, LANES)
                base, (cz, cx, cy) = chosen(k, b, 0)
                for t in range(tiles):
                    line[b, pl.ds(t * TILE, TILE), :] = along_y(base, cz, cy, b, t)
                for t, row in targets:
                    acc = along_x(line, cx, b, t * TILE)
                    out_ref[k, pl.ds(row, TILE), here] = acc
                    for end, end_ref in zip(ends, outputs[1:]):
                        if t == end:
                            end_ref[k, :, here] = acc
                if rim:
                    t, row = rim
                    base, (cz, below_x, cy) = chosen(k, b, 2)
                    for place, tile in [(0, t - 1), (TILE, t)]:
                        brim[b, pl.ds(place, TILE), :] = along_y(base, cz, cy, b, tile)
                    base, (cz, above_x, cy) = chosen(k, b, 1)
                    for place, tile in [(2 * TILE, t), (3 * TILE, t + 1)]:
                        brim[b, pl.ds(place, TILE), :] = along_y(base, cz, cy, b, tile)
                    out_ref[k, pl.ds(row, TILE), here] = jnp.where(
                        from_below, along_x(brim, below_x, b, TILE), along_x(brim, above_x, b, 2 * TILE)
                    )
            if finish:
                for copy in drains(k):
                    copy.start()
            return carry

        lax.fori_loop(0, planes, plane, 0)
        if finish:
            last.wait()
            for k in range(planes):
                for copy in drains(k):
                    copy.wait()

    inside = pl.BlockSpec(memory_space=pltpu.VMEM)
    scalars = pl.BlockSpec(memory_space=pltpu.SMEM)
    scratch = [
        pltpu.VMEM((3 * planes, tiles * TILE, width), jnp.float32),
        pltpu.VMEM((blocks, tiles * TILE, LANES), jnp.float32),
        pltpu.VMEM((blocks, 4 * TILE, LANES), jnp.float32),
    ]
    if finish:
        out_shape = jax.ShapeDtypeStruct((planes, whole, width), jnp.float32)
        out_specs = pl.BlockSpec(memory_space=pl.ANY)
        scratch += [
            pltpu.VMEM((planes, whole, width), jnp.float32),
            pltpu.SemaphoreType.DMA((1 + 2 * planes,)),
        ]
    else:
        height = max(row for _, row in targets) + TILE
        out_shape = [jax.ShapeDtypeStruct((planes, height, width), jnp.float32)]
        out_shape += [jax.ShapeDtypeStruct((planes, TILE, width), jnp.float32)] * len(ends)
        out_specs = [inside] * len(out_shape)
    return pl.pallas_call(
        body,
        out_shape=out_shape,
        in_specs=[scalars] * 2 + [inside] * len(inputs),
        out_specs=out_specs,
        scratch_shapes=scratch,
        compiler_params=pltpu.CompilerParams(vmem_limit_bytes=14 << 20),
        name="sweep",
    )(tags, table, *inputs)


def swapped(x, axis, first):
    devices = lax.axis_size(axis)
    pairs = []
    for i in range(first, devices + first, 2):
        a, b = i % devices, (i + 1) % devices
        pairs += [(a, b), (b, a)]
    return lax.ppermute(x, axis, pairs)


def stacked(x):
    far = swapped(x, "gz", 1)
    near = swapped(x, "gz", 0)
    return x, near, far


def rim_of(first, last):
    even = lax.axis_index("xy") % 2 == 0
    one = swapped(jnp.where(even, last, first), "xy", 0)
    other = swapped(jnp.where(even, first, last), "xy", 1)
    row = lax.broadcasted_iota(jnp.int32, first.shape, 1)
    return jnp.where((row < TILE // 2) == even, one, other)


def advance(image, offsets, frac_index, fractions):
    rows = image.shape[1]
    steps = offsets.shape[0]
    table = weight_table(fractions)
    odd = lax.axis_index("gz").astype(jnp.int32) % 2
    tags = jnp.stack([offsets.reshape(-1), frac_index.reshape(-1)])
    even = lax.axis_index("xy") % 2 == 0
    one, other = swapped(tags, "xy", 0), swapped(tags, "xy", 1)
    above, below = jnp.where(even, other, one), jnp.where(even, one, other)
    tags = jnp.concatenate([tags, above, below, jnp.full((1, offsets.size), odd)])
    margin = MARGIN
    centre = image[:, margin : rows - margin]
    first, last = image[:, :TILE], image[:, rows - TILE :]
    outer = None
    for step in range(steps):
        if step % 2 == 0:
            rim = rim_of(first, last)
            if outer is None:
                outer = jnp.concatenate([image[:, rows - margin :], rim, image[:, :margin]], axis=1)
            else:
                outer = lax.dynamic_update_slice(outer, rim, (0, margin, 0))
        inner = stacked(centre)
        outside = stacked(outer)
        tall = rows - 2 * margin
        many = margin // TILE
        margin += TILE
        (centre,) = sweep(
            step, [inner], [(0, 0, 0, tall)], tall // TILE,
            [(t, (t - 1) * TILE) for t in range(1, tall // TILE - 1)], tags, table,
        )
        moves = [(0, tall - 16, 0, 16), (1, 0, 16, 2 * margin - TILE), (0, 0, 8 + 2 * margin, 16)]
        upper, lower = range(1, many + 2), range(many + 3, 2 * many + 4)
        if step < steps - 1:
            trade = step % 2 == 1
            outer, *edges = sweep(
                step, [inner, outside], moves, 2 * many + 5,
                [(t, (t - 1) * TILE) for t in (*upper, *lower)], tags, table,
                ends=(many + 1, many + 3) if trade else (), rim=None if trade else (many + 2, margin),
            )
            if trade:
                last, first = edges
        else:
            targets = [(t, rows - margin + (t - 1) * TILE) for t in upper]
            targets += [(t, (t - many - 3) * TILE) for t in lower]
            image = sweep(
                step, [inner, outside], moves, 2 * many + 5, targets, tags, table,
                finish=(rows, margin, centre),
            )
    return image


def solution(mesh):
    in_specs = (P("gz", "xy", None), P(None, "gz", "xy", None), P(None, "gz", "xy", None), P())
    out_specs = P("gz", "xy", None)
    return jax.shard_map(advance, mesh=mesh, in_specs=in_specs, out_specs=out_specs, check_vma=False)
```

```python
import jax
import jax.numpy as jnp
from jax import lax
from jax.experimental import pallas as pl
from jax.experimental.pallas import tpu as pltpu
from jax.sharding import PartitionSpec as P


REACH = 8
LANES = 128
TILE = 8
MARGIN = 16


def cubic_weights(shares):
    return (
        -shares * (shares - 1.0) * (shares - 2.0) / 6.0,
        (shares + 1.0) * (shares - 1.0) * (shares - 2.0) / 2.0,
        -(shares + 1.0) * shares * (shares - 2.0) / 2.0,
        (shares + 1.0) * shares * (shares - 1.0) / 6.0,
    )


def weight_table(fractions):
    parts = [jnp.stack(cubic_weights(1.0 - fractions[:, axis]), axis=1) for axis in range(3)]
    return jnp.concatenate(parts, axis=1).reshape(-1)


def sweep(step, pieces, moves, tiles, targets, tags, table, rim=None, finish=None):
    planes, _, width = pieces[0][1].shape
    blocks = width // LANES
    inputs = [part for piece in pieces for part in piece]
    if finish:
        whole, first, middle = finish
        inputs.append(middle)
        after = first + middle.shape[1]

    def body(tag_ref, tab_ref, *refs):
        sources = refs[: len(inputs)]
        result, win, line, brim, *more = refs[len(inputs) :]
        out_ref = result
        if finish:
            out_ref, sems = more
            last = pltpu.make_async_copy(sources[-1], result.at[:, pl.ds(first, after - first), :], sems.at[0])
            last.start()

        def drains(k):
            return [
                pltpu.make_async_copy(
                    out_ref.at[k, pl.ds(row, height), :], result.at[k, pl.ds(row, height), :], sems.at[1 + 2 * k + i]
                )
                for i, (row, height) in enumerate([(0, first), (after, whole - after)])
            ]

        odd = tag_ref[6, 0]
        starts = [planes, 2 * planes * (1 - odd), 2 * planes * odd]

        def fill(p, carry):
            for piece, row, at, height in moves:
                for part in range(3):
                    win[starts[part] + p, pl.ds(at, height), :] = sources[3 * piece + part][p, pl.ds(row, height), :]
            return carry

        lax.fori_loop(0, planes, fill, 0)
        lane = lax.broadcasted_iota(jnp.int32, (TILE, LANES), 1)
        from_right = lane < LANES // 2
        last_two = lane >= LANES - 2
        last_one = lane >= LANES - 1
        first_one = lane == 0

        from_below = lax.broadcasted_iota(jnp.int32, (TILE, LANES), 0) < TILE // 2

        def chosen(k, b, kind):
            tag = (step * planes + k) * blocks + b
            entry = tag_ref[2 * kind + 1, tag] * 12
            weights = [[tab_ref[entry + 4 * axis + n] for n in range(4)] for axis in range(3)]
            return k - tag_ref[2 * kind, tag] + (REACH - 2), weights

        def along_y(base, cz, cy, b, t):
            rows = pl.ds(t * TILE, TILE)
            here = pl.ds(b * LANES, LANES)
            left = pl.ds(((b - 1) % blocks) * LANES, LANES)
            right = pl.ds(((b + 1) % blocks) * LANES, LANES)
            mid = None
            edge = None
            for n in range(4):
                m = cz[n] * win[base + n, rows, here]
                e = cz[n] * jnp.where(from_right, win[base + n, rows, right], win[base + n, rows, left])
                mid = m if mid is None else mid + m
                edge = e if edge is None else edge + e
            y = cy[2] * mid
            y = y + cy[0] * pltpu.roll(jnp.where(last_two, edge, mid), 2, 1)
            y = y + cy[1] * pltpu.roll(jnp.where(last_one, edge, mid), 1, 1)
            return y + cy[3] * pltpu.roll(jnp.where(first_one, edge, mid), LANES - 1, 1)

        def along_x(lines, cx, b, row):
            acc = cx[0] * lines[b, pl.ds(row - 2, TILE), :]
            for n in range(1, 4):
                acc = acc + cx[n] * lines[b, pl.ds(row - 2 + n, TILE), :]
            return acc

        def plane(k, carry):
            for b in range(blocks):
                here = pl.ds(b * LANES, LANES)
                base, (cz, cx, cy) = chosen(k, b, 0)
                for t in range(tiles):
                    line[b, pl.ds(t * TILE, TILE), :] = along_y(base, cz, cy, b, t)
                for t, row in targets:
                    out_ref[k, pl.ds(row, TILE), here] = along_x(line, cx, b, t * TILE)
                if rim:
                    t, row = rim
                    base, (cz, below_x, cy) = chosen(k, b, 2)
                    for place, tile in [(0, t - 1), (TILE, t)]:
                        brim[b, pl.ds(place, TILE), :] = along_y(base, cz, cy, b, tile)
                    base, (cz, above_x, cy) = chosen(k, b, 1)
                    for place, tile in [(2 * TILE, t), (3 * TILE, t + 1)]:
                        brim[b, pl.ds(place, TILE), :] = along_y(base, cz, cy, b, tile)
                    out_ref[k, pl.ds(row, TILE), here] = jnp.where(
                        from_below, along_x(brim, below_x, b, TILE), along_x(brim, above_x, b, 2 * TILE)
                    )
            if finish:
                for copy in drains(k):
                    copy.start()
            return carry

        def two_planes(i, carry):
            return plane(2 * i + 1, plane(2 * i, carry))

        lax.fori_loop(0, planes // 2, two_planes, 0)
        if finish:
            last.wait()
            for k in range(planes):
                for copy in drains(k):
                    copy.wait()

    inside = pl.BlockSpec(memory_space=pltpu.VMEM)
    scalars = pl.BlockSpec(memory_space=pltpu.SMEM)
    scratch = [
        pltpu.VMEM((3 * planes, tiles * TILE, width), jnp.float32),
        pltpu.VMEM((blocks, tiles * TILE, LANES), jnp.float32),
        pltpu.VMEM((blocks, 4 * TILE, LANES), jnp.float32),
    ]
    if finish:
        out_shape = jax.ShapeDtypeStruct((planes, whole, width), jnp.float32)
        out_specs = pl.BlockSpec(memory_space=pl.ANY)
        scratch += [
            pltpu.VMEM((planes, whole, width), jnp.float32),
            pltpu.SemaphoreType.DMA((1 + 2 * planes,)),
        ]
    else:
        height = max(row for _, row in targets) + TILE
        out_shape = [jax.ShapeDtypeStruct((planes, height, width), jnp.float32)]
        out_specs = [inside]
    return pl.pallas_call(
        body,
        out_shape=out_shape,
        in_specs=[scalars] * 2 + [inside] * len(inputs),
        out_specs=out_specs,
        scratch_shapes=scratch,
        compiler_params=pltpu.CompilerParams(vmem_limit_bytes=14 << 20),
        name="sweep",
    )(tags, table, *inputs)


def swapped(x, axis, first):
    devices = lax.axis_size(axis)
    pairs = []
    for i in range(first, devices + first, 2):
        a, b = i % devices, (i + 1) % devices
        pairs += [(a, b), (b, a)]
    return lax.ppermute(x, axis, pairs)


def stacked(x):
    far = swapped(x, "gz", 1)
    near = swapped(x, "gz", 0)
    return x, near, far


def rim_of(first, last):
    even = lax.axis_index("xy") % 2 == 0
    one = swapped(jnp.where(even, last, first), "xy", 0)
    other = swapped(jnp.where(even, first, last), "xy", 1)
    row = lax.broadcasted_iota(jnp.int32, first.shape, 1)
    return jnp.where((row < TILE // 2) == even, one, other)


def advance(image, offsets, frac_index, fractions):
    rows = image.shape[1]
    steps = offsets.shape[0]
    table = weight_table(fractions)
    odd = lax.axis_index("gz").astype(jnp.int32) % 2
    tags = jnp.stack([offsets.reshape(-1), frac_index.reshape(-1)])
    even = lax.axis_index("xy") % 2 == 0
    one, other = swapped(tags, "xy", 0), swapped(tags, "xy", 1)
    above, below = jnp.where(even, other, one), jnp.where(even, one, other)
    tags = jnp.concatenate([tags, above, below, jnp.full((1, offsets.size), odd)])
    margin = MARGIN
    centre = image[:, margin : rows - margin]
    first, last = image[:, :TILE], image[:, rows - TILE :]
    outer = None
    for step in range(steps):
        if step % 2 == 0:
            rim = rim_of(first, last)
            if outer is None:
                outer = jnp.concatenate([image[:, rows - margin :], rim, image[:, :margin]], axis=1)
            else:
                outer = lax.dynamic_update_slice(outer, rim, (0, margin, 0))
        inner = stacked(centre)
        outside = stacked(outer)
        tall = rows - 2 * margin
        many = margin // TILE
        margin += TILE
        (centre,) = sweep(
            step, [inner], [(0, 0, 0, tall)], tall // TILE,
            [(t, (t - 1) * TILE) for t in range(1, tall // TILE - 1)], tags, table,
        )
        moves = [(0, tall - 16, 0, 16), (1, 0, 16, 2 * margin - TILE), (0, 0, 8 + 2 * margin, 16)]
        upper, lower = range(1, many + 2), range(many + 3, 2 * many + 4)
        trade = step % 2 == 1 and step < steps - 1
        if trade:
            (ends,) = sweep(
                step, [outside], [(0, margin - TILE - 16, 0, 40)], 5, [(1, 0), (3, TILE)], tags, table,
            )
            last, first = ends[:, :TILE], ends[:, TILE:]
        if step < steps - 1:
            (outer,) = sweep(
                step, [inner, outside], moves, 2 * many + 5,
                [(t, (t - 1) * TILE) for t in (*upper, *lower)], tags, table,
                rim=None if trade else (many + 2, margin),
            )
        else:
            targets = [(t, rows - margin + (t - 1) * TILE) for t in upper]
            targets += [(t, (t - many - 3) * TILE) for t in lower]
            image = sweep(
                step, [inner, outside], moves, 2 * many + 5, targets, tags, table,
                finish=(rows, margin, centre),
            )
    return image


def solution(mesh):
    in_specs = (P("gz", "xy", None), P(None, "gz", "xy", None), P(None, "gz", "xy", None), P())
    out_specs = P("gz", "xy", None)
    return jax.shard_map(advance, mesh=mesh, in_specs=in_specs, out_specs=out_specs, check_vma=False)
```
